32 devices in a mesh: pop: 16 (over z, y, core), shard: 2 (over x).
Axes of the slice: x: 2, y: 2, z: 4, core: 2. Of those that a mesh axis runs over, the one named last changes fastest.
Arguments:
- hidden: bfloat16 [2048, 4096], P('pop'), may hold values from -6 to 6
- weight: bfloat16 [4096, 14336], P('pop', 'shard'), may hold values from -0.09375 to 0.09375
- left_factors: bfloat16 [128, 4096], P('pop'), may hold values from -6 to 6
- right_factors: bfloat16 [128, 14336], P('pop', 'shard'), may hold values from -6 to 6
- target: bfloat16 [2048, 14336], P('pop', 'shard'), may hold values from -6 to 6
Outputs:
- up_out: bfloat16 [2048, 14336], P('pop', 'shard')
- step: float32 [4096, 14336], P('pop', 'shard')
- fitness: float32 [128], P('pop')
The draws below stay inside these ranges and needn't reach their ends.
All inputs are finite; a program needn't handle non-finite values.
Results may differ from the reference program's by a relative error of at most 0.001.
Values may be sent and summed in bfloat16 or wider, within the bound.
A program may use at most 128 MiB of HBM per device.

```python
import math
import jax
import jax.numpy as jnp
from jax import lax

D = 4096
FF = 14336
TOK = 16
MEMBERS = 128
ROWS = 2048


def block_scale(rng, dims, cuts, low, top_value):
    def one(dim, shards_of):
        draws = jax.random.uniform(jax.random.fold_in(jax.random.fold_in(rng, 6), dim), (shards_of,), jnp.float32, low / len(cuts), top_value / len(cuts))
        return jnp.repeat(jnp.exp(draws), dims[dim] // shards_of).reshape((-1,) + (1,) * (len(dims) - dim - 1))

    level = one(*cuts[0])
    for cut in cuts[1:]:
        level = level * one(*cut)
    return level


def bell_draw(own_key, extent, scale, limit, split=(), dtype=jnp.bfloat16):
    array = scale * jax.random.normal(own_key, extent, jnp.float32)
    if split:
        array = array * block_scale(own_key, extent, split, -0.22, 0.18)
    return jnp.clip(array, -limit, limit).astype(dtype)


def setup_inputs(seed: int = 0) -> dict:
    seeds = jax.random.split(jax.random.key(seed), 6)
    hidden = bell_draw(seeds[0], (ROWS, D), 1.0, 6.0, ((0, 16),))
    weight = bell_draw(seeds[1], (D, FF), D ** -0.5, 0.09375, ((0, 16), (1, 2)))
    left_factors = bell_draw(seeds[2], (MEMBERS, D), 1.0, 6.0, ((0, 16),))
    right_factors = bell_draw(seeds[3], (MEMBERS, FF), 1.0, 6.0, ((0, 16), (1, 2)))
    target = bell_draw(seeds[4], (ROWS, FF), 1.0, 6.0, ((0, 16), (1, 2)))
    return {"hidden": hidden, "weight": weight, "left_factors": left_factors, "right_factors": right_factors, "target": target}


noise_scale = 0.5
spread_eps = 1e-05

def reference(hidden, weight, left_factors, right_factors, target):
    base_out = jnp.dot(hidden, weight, preferred_element_type=jnp.float32)
    grouped = hidden.reshape(MEMBERS, TOK, D).astype(jnp.float32)
    projected = jnp.einsum('mtd,md->mt', grouped, left_factors.astype(jnp.float32)) / math.sqrt(D)
    right_wide = right_factors.astype(jnp.float32)
    perturbed = base_out.reshape(MEMBERS, TOK, FF) + noise_scale * projected[:, :, None] * right_wide[:, None, :]
    up_out = perturbed.astype(jnp.bfloat16).reshape(ROWS, FF)
    directions = target.reshape(MEMBERS, TOK, FF).astype(jnp.float32)
    reward = lax.optimization_barrier(jnp.sum(jax.nn.silu(perturbed) * directions, axis=(1, 2)))
    mean_reward = jnp.sum(reward) / MEMBERS
    centered = reward - mean_reward
    spread = jnp.sum(centered * centered) / MEMBERS
    fitness = centered / jnp.sqrt(spread + spread_eps)
    weighted = left_factors.astype(jnp.float32) * fitness[:, None]
    summed = lax.dot_general(weighted, right_wide, (((0,), (0,)), ((), ())), precision=lax.Precision.HIGHEST)
    step = summed / math.sqrt(MEMBERS)
    return (up_out, step, fitness)
```

```python
import functools
import math

import jax
import jax.numpy as jnp
from jax import lax
from jax.experimental import pallas as pl
from jax.experimental.pallas import tpu as pltpu
from jax.sharding import PartitionSpec as P

noise_scale = 0.5
spread_eps = 1e-05
lane = 128


def group_size(pop, cols):
    size = 1
    while size * 2 <= min(pop, 8) and cols % (size * 2 * lane) == 0:
        size *= 2
    return size


def high_bits(size):
    bits = []
    bit = size // 2
    while bit:
        bits.append(bit)
        bit //= 2
    return bits


def spans(bits):
    held = [0]
    out = []
    for bit in bits:
        out.append((bit, list(held)))
        held = held + [m ^ bit for m in held]
    return out


def greet(me, shard, pop_masks, shard_masks):
    barrier = pltpu.get_barrier_semaphore()
    for mask in pop_masks:
        pl.semaphore_signal(barrier, inc=1, device_id={"pop": me ^ mask},
                            device_id_type=pl.DeviceIdType.MESH)
    for mask in shard_masks:
        pl.semaphore_signal(barrier, inc=1, device_id={"shard": shard ^ mask},
                            device_id_type=pl.DeviceIdType.MESH)
    pl.semaphore_wait(barrier, len(pop_masks) + len(shard_masks))


def gather_kernel(pop, shards, group, counts,
                  hidden, weight, left, right, target,
                  hidden_all, weight_all, left_all, right_all, target_all,
                  h_send, h_recv, w_send, w_recv, l_send, l_recv,
                  r_send, r_recv, t_send, t_recv, own_sem):
    me = lax.axis_index("pop")
    shard = lax.axis_index("shard")
    rank = lax.rem(me, group)
    rows = hidden.shape[0]
    piece = rows // shards
    cols = weight.shape[1] // group

    def remote(src, dst, send, recv, **where):
        copy = pltpu.make_async_remote_copy(
            src_ref=src, dst_ref=dst, send_sem=send, recv_sem=recv,
            device_id=where, device_id_type=pl.DeviceIdType.MESH)
        copy.start()
        return copy

    def block_of(r):
        return pl.ds(pl.multiple_of(r * cols, lane), cols)

    started = []
    own = [
        (hidden, hidden_all.at[rank]),
        (weight.at[:, block_of(rank)], weight_all.at[me]),
        (left, left_all.at[me]),
        (right, right_all.at[me]),
        (target.at[:, block_of(rank)], target_all.at[rank]),
    ]

    greet(me, shard, list(range(1, pop)), list(range(1, shards)))

    part = pl.ds(pl.multiple_of(shard * piece, piece), piece)
    group_bits = high_bits(group)
    outer_bits = [b for b in group_bits if b > 1]
    inner_bits = [b for b in group_bits if b == 1]

    weight_order = sorted(range(1, pop), key=lambda k: -(k >> 1))
    weight_queue = list(weight_order)

    def push_weight(n):
        for _ in range(n):
            if not weight_queue:
                return
            k = weight_queue.pop(0)
            other = me ^ k
            started.append(remote(
                weight.at[:, block_of(lax.rem(other, group))], weight_all.at[me],
                w_send.at[k - 1], w_recv.at[k - 1], pop=other))

    hid = [0]

    def hidden_copy(mask, rows_of, **where):
        i = hid[0]
        hid[0] += 1
        r = rank ^ mask
        src = hidden if mask == 0 else hidden_all.at[r]
        dst = hidden_all.at[r]
        if rows_of is not None:
            src, dst = src.at[rows_of], dst.at[rows_of]
        return remote(src, dst, h_send.at[i], h_recv.at[i], **where)

    fac = [0]

    def factor_copies(bit, held):
        out = []
        for mask in held:
            i = fac[0]
            fac[0] += 1
            r = me ^ mask
            out.append(remote(left if mask == 0 else left_all.at[r], left_all.at[r],
                              l_send.at[i], l_recv.at[i], pop=me ^ bit))
            out.append(remote(right if mask == 0 else right_all.at[r], right_all.at[r],
                              r_send.at[i], r_recv.at[i], pop=me ^ bit))
        return out

    outer = spans(outer_bits)
    factor_steps = spans(high_bits(pop))
    held_all = [0]
    for bit in outer_bits:
        held_all = held_all + [m ^ bit for m in held_all]

    wait_factor = []
    local = []
    for i in range(max(len(outer), 1)):
        mine = []
        if i < len(outer):
            bit, held = outer[i]
            for mask in held:
                mine.append(hidden_copy(mask, part, pop=me ^ bit))
        for c in wait_factor:
            c.wait_recv()
        if i < len(factor_steps):
            wait_factor = factor_copies(*factor_steps[i])
            started.extend(wait_factor)
        push_weight(4)
        if i == 0:
            for j, (src, dst) in enumerate(own):
                copy = pltpu.make_async_copy(src, dst, own_sem.at[j])
                copy.start()
                local.append(copy)
            for k in range(1, group):
                started.append(remote(
                    target.at[:, block_of(rank ^ k)], target_all.at[rank],
                    t_send.at[k - 1], t_recv.at[k - 1], pop=me ^ k))
        for c in mine:
            c.wait_recv()
        started.extend(mine)
    cross = []
    for j in range(1, shards):
        for mask in held_all[1:]:
            cross.append(hidden_copy(mask, part, shard=shard ^ j))
    for step in factor_steps[max(len(outer), 1):]:
        for c in wait_factor:
            c.wait_recv()
        wait_factor = factor_copies(*step)
        started.extend(wait_factor)
        push_weight(3)
    push_weight(len(weight_queue))
    for c in cross:
        c.wait_recv()
    started.extend(cross)
    last = []
    for bit in inner_bits:
        for mask in held_all:
            last.append(hidden_copy(mask, None, pop=me ^ bit))
    for c in last + wait_factor:
        c.wait_recv()
    started.extend(last)
    for c in started:
        c.wait_send()
    for k in range(1, pop):
        pltpu.make_async_remote_copy(
            src_ref=weight.at[:, block_of(rank)], dst_ref=weight_all.at[me ^ k],
            send_sem=w_send.at[k - 1], recv_sem=w_recv.at[k - 1],
            device_id={"pop": me ^ k}, device_id_type=pl.DeviceIdType.MESH).wait_recv()
    for k in range(1, group):
        pltpu.make_async_remote_copy(
            src_ref=target.at[:, block_of(rank)], dst_ref=target_all.at[rank ^ k],
            send_sem=t_send.at[k - 1], recv_sem=t_recv.at[k - 1],
            device_id={"pop": me ^ k}, device_id_type=pl.DeviceIdType.MESH).wait_recv()
    for c in local:
        c.wait()


def return_kernel(group, blocks, out, send, recv, own_sem):
    me = lax.axis_index("pop")
    rank = lax.rem(me, group)
    cols = blocks.shape[2]
    place = pl.ds(pl.multiple_of(rank * cols, lane), cols)
    local = pltpu.make_async_copy(blocks.at[rank], out.at[:, place], own_sem)
    local.start()
    greet(me, 0, list(range(1, group)), [])
    copies = []
    for k in reversed(range(1, group)):
        copy = pltpu.make_async_remote_copy(
            src_ref=blocks.at[rank ^ k], dst_ref=out.at[:, place],
            send_sem=send.at[k - 1], recv_sem=recv.at[k - 1],
            device_id={"pop": me ^ k}, device_id_type=pl.DeviceIdType.MESH)
        copy.start()
        copies.append(copy)
    for copy in copies:
        copy.wait()
    local.wait()


def split_parts(values):
    high = values.astype(jnp.bfloat16)
    kept = lax.optimization_barrier(high)
    low = (values - kept.astype(jnp.float32)).astype(jnp.bfloat16)
    return (high, low)


def local(hidden, weight, left_factors, right_factors, target):
    pop = lax.axis_size("pop")
    shards = lax.axis_size("shard")
    members, features = left_factors.shape
    rows = hidden.shape[0]
    tokens = rows // members
    depth, local_cols = weight.shape
    group = group_size(pop, local_cols)
    cols = local_cols // group
    member_count = members * pop
    me = lax.axis_index("pop")
    base = (me // group) * group

    anyspace = pl.BlockSpec(memory_space=pl.ANY)
    dma = pltpu.SemaphoreType.DMA
    half = max(group // 2, 1)
    hcount = (half - 1) + (half - 1) * (shards - 1) + (half if group > 1 else 0)
    hcount = max(hcount, 1)
    tcount = max(group - 1, 1)
    fcount = max(pop - 1, 1)
    bf16 = jnp.bfloat16
    hidden_all, weight_all, left_all, right_all, target_all = pl.pallas_call(
        functools.partial(gather_kernel, pop, shards, group, None),
        out_shape=(
            jax.ShapeDtypeStruct((group, rows, features), bf16),
            jax.ShapeDtypeStruct((pop, depth, cols), bf16),
            jax.ShapeDtypeStruct((pop, members, features), bf16),
            jax.ShapeDtypeStruct((pop, members, local_cols), bf16),
            jax.ShapeDtypeStruct((group, rows, cols), bf16),
        ),
        in_specs=[anyspace] * 5,
        out_specs=[anyspace] * 5,
        scratch_shapes=[
            dma((hcount,)), dma((hcount,)), dma((fcount,)), dma((fcount,)),
            dma((fcount,)), dma((fcount,)), dma((fcount,)), dma((fcount,)),
            dma((tcount,)), dma((tcount,)), dma((5,)),
        ],
        compiler_params=pltpu.CompilerParams(collective_id=0, has_side_effects=True),
    )(hidden, weight, left_factors, right_factors, target)

    group_members = group * members
    base_out = jnp.dot(
        hidden_all.reshape(group * rows, features),
        weight_all.reshape(pop * depth, cols),
        preferred_element_type=jnp.float32,
    )
    left_group = lax.dynamic_slice_in_dim(left_all, base, group, 0)
    right_group = lax.dynamic_slice(
        right_all, (base, 0, (me % group) * cols), (group, members, cols)
    ).reshape(group_members, cols)
    projected = jnp.einsum(
        "mtd,md->mt",
        hidden_all.reshape(group_members, tokens, features),
        left_group.reshape(group_members, features),
        preferred_element_type=jnp.float32,
    ) / math.sqrt(features)
    perturbed = (
        base_out.reshape(group_members, tokens, cols)
        + noise_scale * projected[:, :, None] * right_group.astype(jnp.float32)[:, None, :]
    )
    blocks = perturbed.astype(bf16).reshape(group, rows, cols)
    directions = target_all.reshape(group_members, tokens, cols).astype(jnp.float32)
    partial_value = jnp.sum(jax.nn.silu(perturbed) * directions, axis=(1, 2))
    placed = lax.dynamic_update_slice_in_dim(
        jnp.zeros((member_count,), jnp.float32), partial_value, base * members, 0)
    reward = lax.psum(placed, ("pop", "shard"))

    up_out = pl.pallas_call(
        functools.partial(return_kernel, group),
        out_shape=jax.ShapeDtypeStruct((rows, local_cols), bf16),
        in_specs=[anyspace],
        out_specs=anyspace,
        scratch_shapes=[dma((tcount,)), dma((tcount,)), dma(())],
        compiler_params=pltpu.CompilerParams(collective_id=1, has_side_effects=True),
    )(blocks)

    centered = reward - jnp.sum(reward) / member_count
    spread = jnp.sum(centered * centered) / member_count
    fitness_all = centered / jnp.sqrt(spread + spread_eps)
    fitness = lax.dynamic_slice_in_dim(fitness_all, me * members, members, 0)
    left_mine = lax.dynamic_slice_in_dim(
        left_all.reshape(member_count, features), me * depth, depth, 1)
    weighted = left_mine.astype(jnp.float32) * fitness_all[:, None]
    high, low = split_parts(weighted)
    contract = (((0,), (0,)), ((), ()))
    portion = right_all.reshape(member_count, local_cols)
    upper = lax.dot_general(high, portion, contract, preferred_element_type=jnp.float32)
    lower = lax.dot_general(low, portion, contract, preferred_element_type=jnp.float32)
    step = (upper + lower) / math.sqrt(member_count)
    return (up_out, step, fitness)


def solution(mesh):
    in_specs = (
        P("pop", None),
        P("pop", "shard"),
        P("pop", None),
        P("pop", "shard"),
        P("pop", "shard"),
    )
    out_specs = (P("pop", "shard"), P("pop", "shard"), P("pop"))
    return jax.shard_map(local, mesh=mesh, in_specs=in_specs, out_specs=out_specs, check_vma=False)
```

```python
import functools
import math

import jax
import jax.numpy as jnp
from jax import lax
from jax.experimental import pallas as pl
from jax.experimental.pallas import tpu as pltpu
from jax.sharding import PartitionSpec as P

noise_scale = 0.5
spread_eps = 1e-05
lane = 128


def group_size(pop, cols):
    size = 1
    while size * 2 <= min(pop, 8) and cols % (size * 2 * lane) == 0:
        size *= 2
    return size


def high_bits(size):
    bits = []
    bit = size // 2
    while bit:
        bits.append(bit)
        bit //= 2
    return bits


def spans(bits):
    held = [0]
    out = []
    for bit in bits:
        out.append((bit, list(held)))
        held = held + [m ^ bit for m in held]
    return out


def greet(me, shard, pop_masks, shard_masks):
    barrier = pltpu.get_barrier_semaphore()
    for mask in pop_masks:
        pl.semaphore_signal(barrier, inc=1, device_id={"pop": me ^ mask},
                            device_id_type=pl.DeviceIdType.MESH)
    for mask in shard_masks:
        pl.semaphore_signal(barrier, inc=1, device_id={"shard": shard ^ mask},
                            device_id_type=pl.DeviceIdType.MESH)
    pl.semaphore_wait(barrier, len(pop_masks) + len(shard_masks))


def chunks_of(cols):
    out = []
    start = 0
    while start < cols:
        width = min(2 * lane, cols - start)
        out.append((start, width))
        start += width
    return out


def fused_kernel(pop, shards, group, tokens,
                 hidden, weight, left, right, target,
                 up_out, left_all, right_all, rewards,
                 hidden_v, weight_v, target_v, up_v, left_v, right_v, proj_v, racc, rsum, rmine, rall,
                 h_send, h_recv, w_send, w_recv, l_send, l_recv,
                 r_send, r_recv, t_send, t_recv, u_send, u_recv,
                 s_send, s_recv, p_send, p_recv, own_sem, own_up, pre_sem):
    me = lax.axis_index("pop")
    shard = lax.axis_index("shard")
    rank = lax.rem(me, group)
    base = me - rank
    rows, features = hidden.shape
    members = left.shape[0]
    depth = weight.shape[0]
    piece = rows // shards
    cols = weight.shape[1] // group
    chunks = chunks_of(cols)

    def remote(src, dst, send, recv, **where):
        return pltpu.make_async_remote_copy(
            src_ref=src, dst_ref=dst, send_sem=send, recv_sem=recv,
            device_id=where, device_id_type=pl.DeviceIdType.MESH)

    def columns(r, start, width):
        return pl.ds(pl.multiple_of(r * cols + start, lane), width)

    def row_block(r, size=rows):
        return pl.ds(pl.multiple_of(r * size, size), size)

    started = []

    def go(copy):
        copy.start()
        started.append(copy)
        return copy

    greet(me, shard, list(range(1, pop)), list(range(1, shards)))

    local = [
        pltpu.make_async_copy(hidden, hidden_v.at[row_block(rank), :], own_sem.at[0]),
        pltpu.make_async_copy(weight.at[:, columns(rank, 0, cols)],
                              weight_v.at[row_block(me, depth), :], own_sem.at[1]),
        pltpu.make_async_copy(left, left_all.at[me], own_sem.at[2]),
        pltpu.make_async_copy(right, right_all.at[me], own_sem.at[3]),
        pltpu.make_async_copy(target.at[:, columns(rank, 0, cols)],
                              target_v.at[row_block(rank), :], own_sem.at[4]),
    ]

    group_bits = high_bits(group)
    outer = spans([b for b in group_bits if b > 1])
    held_all = [0]
    for bit, _ in outer:
        held_all = held_all + [m ^ bit for m in held_all]
    factor_steps = spans(high_bits(pop))
    order = sorted(range(1, pop), key=lambda k: -(k >> 1))

    def weight_copy(c, k, sender):
        start, width = chunks[c]
        there = pl.ds(start, width)
        return remote(
            weight.at[:, columns(lax.rem(me ^ k, group), start, width)],
            weight_v.at[row_block(sender, depth), there],
            w_send.at[c * (pop - 1) + k - 1], w_recv.at[c * (pop - 1) + k - 1], pop=me ^ k)

    def push_weights(c):
        if c < len(chunks):
            for k in order:
                go(weight_copy(c, k, me))

    def target_copy(k, sender_rank):
        return remote(
            target.at[:, columns(rank ^ k, 0, cols)], target_v.at[row_block(sender_rank), :],
            t_send.at[k - 1], t_recv.at[k - 1], pop=me ^ k)

    counts = [0, 0]

    def hidden_copy(mask, full, **where):
        i = counts[0]
        counts[0] += 1
        r = rank ^ mask
        size, first = (rows, 0) if full else (piece, shard * piece)
        src = (hidden.at[pl.ds(pl.multiple_of(first, size), size), :] if mask == 0 else
               hidden_v.at[pl.ds(pl.multiple_of(r * rows + first, size), size), :])
        dst = hidden_v.at[pl.ds(pl.multiple_of(r * rows + first, size), size), :]
        return go(remote(src, dst, h_send.at[i], h_recv.at[i], **where))

    def factor_copies(bit, held):
        out = []
        for mask in held:
            i = counts[1]
            counts[1] += 1
            r = me ^ mask
            out.append(go(remote(left if mask == 0 else left_all.at[r], left_all.at[r],
                                 l_send.at[i], l_recv.at[i], pop=me ^ bit)))
            out.append(go(remote(right if mask == 0 else right_all.at[r], right_all.at[r],
                                 r_send.at[i], r_recv.at[i], pop=me ^ bit)))
        return out

    def arrived(copies):
        for c in copies:
            c.wait_recv()

    pushed = 0
    waiting = []
    for i, (bit, held) in enumerate(outer):
        mine = [hidden_copy(mask, False, pop=me ^ bit) for mask in held]
        arrived(waiting)
        waiting = factor_copies(*factor_steps[i])
        push_weights(pushed)
        pushed += 1
        if i == 0:
            for copy in local:
                copy.start()
            for k in range(1, group):
                go(target_copy(k, rank))
        arrived(mine)
    cross = [hidden_copy(mask, False, shard=shard ^ j)
             for j in range(1, shards) for mask in held_all[1:]]
    if not outer:
        for copy in local:
            copy.start()
        for k in range(1, group):
            go(target_copy(k, rank))
    for step in factor_steps[len(outer):]:
        arrived(waiting)
        waiting = factor_copies(*step)
        push_weights(pushed)
        pushed += 1
    while pushed < len(chunks):
        push_weights(pushed)
        pushed += 1
    arrived(cross)
    last = [hidden_copy(mask, True, pop=me ^ 1) for mask in held_all]
    arrived(waiting)
    for copy in local:
        copy.wait()
    near = [
        pltpu.make_async_copy(left_all.at[pl.ds(base, group)], left_v, pre_sem.at[0]),
        pltpu.make_async_copy(right_all.at[pl.ds(base, group), :, columns(rank, 0, cols)],
                              right_v, pre_sem.at[1]),
    ]
    for copy in near:
        copy.start()
    for copy in near:
        copy.wait()
    arrived(last)
    for k in range(1, group):
        target_copy(k, rank ^ k).wait_recv()

    half = group * rows // 2
    half_members = half // tokens
    total_members = group * members
    left_rows = left_v[...].astype(jnp.float32).reshape(total_members, features).astype(jnp.bfloat16)

    def project(h, carry):
        at = pl.ds(pl.multiple_of(h * half, half), half)
        full = lax.dot_general(hidden_v[at, :], left_rows, (((1,), (1,)), ((), ())),
                               preferred_element_type=jnp.float32)
        row = lax.broadcasted_iota(jnp.int32, full.shape, 0) + h * half
        member = lax.broadcasted_iota(jnp.int32, full.shape, 1)
        first = member * tokens
        keep = (row >= first) & (row < first + tokens)
        proj_v[at, :] = (noise_scale / math.sqrt(features)) * jnp.sum(
            jnp.where(keep, full, 0.0), axis=1, keepdims=True)
        return carry

    lax.fori_loop(0, 2, project, 0)
    racc[...] = jnp.zeros_like(racc)

    for c, (start, width) in enumerate(chunks):
        for k in order:
            weight_copy(c, k, me ^ k).wait_recv()
        span = pl.ds(start, width)

        def compute(h, carry, span=span, width=width):
            at = pl.ds(pl.multiple_of(h * half, half), half)
            base_out = jnp.dot(hidden_v[at, :], weight_v[:, span],
                               preferred_element_type=jnp.float32)
            wide = right_v[pl.ds(h * (group // 2), group // 2), :, span].astype(jnp.float32)
            wide = wide.reshape(half_members, width)
            wide = jnp.broadcast_to(wide[:, None, :], (half_members, tokens, width))
            perturbed = base_out + proj_v[at, :] * wide.reshape(half, width)
            up_v[at, span] = perturbed.astype(jnp.bfloat16)
            term = perturbed / (1.0 + jnp.exp(-perturbed)) * target_v[at, span].astype(jnp.float32)
            summed = jnp.sum(term.reshape(half_members, tokens, width), axis=1)
            line = summed[:, :lane]
            for j in range(1, width // lane):
                line = line + summed[:, j * lane:(j + 1) * lane]
            mine = pl.ds(pl.multiple_of(h * half_members, half_members), half_members)
            racc[mine, :] = racc[mine, :] + line
            return carry

        lax.fori_loop(0, 2, compute, 0)
        for k in reversed(range(1, group)):
            i = c * (group - 1) + k - 1
            go(remote(up_v.at[row_block(rank ^ k), span], up_out.at[:, columns(rank, start, width)],
                      u_send.at[i], u_recv.at[i], pop=me ^ k))
        copy = pltpu.make_async_copy(up_v.at[row_block(rank), span],
                                     up_out.at[:, columns(rank, start, width)], own_up.at[c])
        copy.start()
        local.append(copy)

    line = jnp.sum(jnp.transpose(racc[...]), axis=0, keepdims=True)
    rmine[...] = jnp.zeros_like(rmine)
    rmine[0:1, 0:total_members] = line[:, :total_members]
    ahead = [go(remote(rmine, rsum.at[j - 1], s_send.at[j - 1], s_recv.at[j - 1], shard=shard ^ j))
             for j in range(1, shards)]
    arrived(ahead)
    value = rmine[...]
    for j in range(1, shards):
        value = value + rsum[j - 1]
    rall[me] = value
    out = [go(remote(rall.at[me], rall.at[me], p_send.at[k - 1], p_recv.at[k - 1], pop=me ^ k))
           for k in range(1, pop)]
    for k in range(1, pop):
        remote(rall.at[me], rall.at[me ^ k], p_send.at[k - 1], p_recv.at[k - 1],
               pop=me ^ k).wait_recv()
    for c in range(len(chunks)):
        start, width = chunks[c]
        for k in range(1, group):
            i = c * (group - 1) + k - 1
            remote(up_v.at[row_block(rank ^ k), pl.ds(start, width)],
                   up_out.at[:, columns(rank ^ k, start, width)],
                   u_send.at[i], u_recv.at[i], pop=me ^ k).wait_recv()
    for copy in started:
        copy.wait_send()
    for copy in local[5:]:
        copy.wait()
    rewards[...] = rall[...]


def split_parts(values):
    high = values.astype(jnp.bfloat16)
    kept = lax.optimization_barrier(high)
    low = (values - kept.astype(jnp.float32)).astype(jnp.bfloat16)
    return (high, low)


def local(hidden, weight, left_factors, right_factors, target):
    pop = lax.axis_size("pop")
    shards = lax.axis_size("shard")
    members, features = left_factors.shape
    rows = hidden.shape[0]
    tokens = rows // members
    depth, local_cols = weight.shape
    group = group_size(pop, local_cols)
    cols = local_cols // group
    member_count = members * pop
    me = lax.axis_index("pop")

    anyspace = pl.BlockSpec(memory_space=pl.ANY)
    dma = pltpu.SemaphoreType.DMA
    half = group // 2
    hcount = (half - 1) * shards + half
    tcount = group - 1
    fcount = pop - 1
    nchunks = len(chunks_of(cols))
    bf16 = jnp.bfloat16
    group_rows = group * rows
    scratch = [
        pltpu.VMEM((group_rows, features), bf16),
        pltpu.VMEM((pop * depth, cols), bf16),
        pltpu.VMEM((group_rows, cols), bf16),
        pltpu.VMEM((group_rows, cols), bf16),
        pltpu.VMEM((group, members, features), bf16),
        pltpu.VMEM((group, members, cols), bf16),
        pltpu.VMEM((group_rows, 1), jnp.float32),
        pltpu.VMEM((group * members, lane), jnp.float32),
        pltpu.VMEM((max(shards - 1, 1), 8, lane), jnp.float32),
        pltpu.VMEM((8, lane), jnp.float32),
        pltpu.VMEM((pop, 8, lane), jnp.float32),
    ]
    for count in (hcount, nchunks * fcount, fcount, fcount, tcount, nchunks * tcount,
                  max(shards - 1, 1), fcount):
        scratch += [dma((count,)), dma((count,))]
    scratch += [dma((5,)), dma((nchunks,)), dma((2,))]
    up_out, left_all, right_all, rewards = pl.pallas_call(
        functools.partial(fused_kernel, pop, shards, group, tokens),
        out_shape=(
            jax.ShapeDtypeStruct((rows, local_cols), bf16),
            jax.ShapeDtypeStruct((pop, members, features), bf16),
            jax.ShapeDtypeStruct((pop, members, local_cols), bf16),
            jax.ShapeDtypeStruct((pop, 8, lane), jnp.float32),
        ),
        in_specs=[anyspace] * 5,
        out_specs=[anyspace] * 3 + [pl.BlockSpec(memory_space=pltpu.VMEM)],
        scratch_shapes=scratch,
        compiler_params=pltpu.CompilerParams(
            collective_id=0, has_side_effects=True, vmem_limit_bytes=60 * 1024 * 1024),
    )(hidden, weight, left_factors, right_factors, target)
    group_members = group * members
    reward = jnp.sum(
        rewards[:, 0, :group_members].reshape(pop // group, group, group_members), axis=1
    ).reshape(member_count)

    centered = reward - jnp.sum(reward) / member_count
    spread = jnp.sum(centered * centered) / member_count
    fitness_all = centered / jnp.sqrt(spread + spread_eps)
    fitness = lax.dynamic_slice_in_dim(fitness_all, me * members, members, 0)
    left_mine = lax.dynamic_slice_in_dim(
        left_all.reshape(member_count, features), me * depth, depth, 1)
    weighted = left_mine.astype(jnp.float32) * fitness_all[:, None]
    high, low = split_parts(weighted)
    contract = (((0,), (0,)), ((), ()))
    portion = right_all.reshape(member_count, local_cols)
    upper = lax.dot_general(high, portion, contract, preferred_element_type=jnp.float32)
    lower = lax.dot_general(low, portion, contract, preferred_element_type=jnp.float32)
    step = (upper + lower) / math.sqrt(member_count)
    return (up_out, step, fitness)


def solution(mesh):
    in_specs = (
        P("pop", None),
        P("pop", "shard"),
        P("pop", None),
        P("pop", "shard"),
        P("pop", "shard"),
    )
    out_specs = (P("pop", "shard"), P("pop", "shard"), P("pop"))
    return jax.shard_map(local, mesh=mesh, in_specs=in_specs, out_specs=out_specs, check_vma=False)
```
